256 devices in a mesh: win: 2 (over y), row: 128 (over x, z, core).
Axes of the slice: x: 4, y: 2, z: 16, core: 2. Of those that a mesh axis runs over, the one named last changes fastest.
The devices are a block of a 4x16x16 slice.
Arguments:
- spectra: bfloat16 [256, 2, 32768], P(('win', 'row')), parts along dimension 0, may hold values from -6 to 6
- pair_mask: int32 [128, 128], P('row'), may hold values from 0 to 1, as said below
- available: int32 [256], P('win'), parts along dimension 0, may hold values 0 or 1
Outputs:
- correlations: float32 [256, 128, 8192], P(('win', 'row')), parts along dimension 0
The draws below stay inside these ranges and needn't reach their ends.
There are 2 independent parts, one for each index of `win`. The reference program is written for one: setup_inputs(seed, part) draws one part's arguments, and reference() takes and returns one part's arrays. A program takes and returns all parts, laid end to end along the dimension named above; an argument that names none is the same for every part. Nothing has to cross between parts.
Inputs may be any that keep to these rules, and one draw needn't show every extreme that they name: pair_mask[i, j] is 0 wherever j <= i.
All inputs are finite; a program needn't handle non-finite values.
Results may differ from the reference program's by a relative error of at most 0.0003.
Values may be sent and summed in bfloat16 or wider, within the bound.
No kernel may reach another device: no remote copies, remote signals or barrier semaphores. Data moves between devices by JAX's collectives and lax.ppermute only.
A program may use at most 128 MiB of HBM per device.

```python
import math
import jax
import jax.numpy as jnp
from jax import lax

STATIONS = 128
FREQ = 32768
LAGS = 8192


def draw_pair_mask(key, part):
    picks = jax.random.randint(key, (STATIONS, STATIONS), 0, 4)
    rows = lax.broadcasted_iota(jnp.int32, (STATIONS, STATIONS), 0)
    cols = lax.broadcasted_iota(jnp.int32, (STATIONS, STATIONS), 1)
    return jnp.where((cols > rows) & (picks < 3), 1, 0).astype(jnp.int32)


def place_ends(result, key, low, largest):
    dims = result.shape
    place = [jax.random.randint(jax.random.fold_in(key, axis), (), 0, dims[axis]) for axis in range(len(dims))]
    result = result.at[tuple(place)].set(low)
    longest = dims.index(max(dims))
    place[longest] = (place[longest] + 1) % dims[longest]
    return result.at[tuple(place)].set(largest)


def level_of(own_key, extent, cuts, low, largest):
    def one(axis_at, parts):
        steps = jax.random.uniform(jax.random.fold_in(jax.random.fold_in(own_key, 6), axis_at), (parts,), jnp.float32, low / len(cuts), largest / len(cuts))
        return jnp.repeat(jnp.exp(steps), extent[axis_at] // parts).reshape((-1,) + (1,) * (len(extent) - axis_at - 1))

    gain = one(*cuts[0])
    for cut in cuts[1:]:
        gain = gain * one(*cut)
    return gain


def normal_values(key, shape, spread, bound, shards=(), held_as=jnp.bfloat16):
    values = spread * jax.random.normal(key, shape, jnp.float32)
    if shards:
        values = values * level_of(key, shape, shards, -0.22, 0.18)
    return jnp.clip(values, -bound, bound).astype(held_as)


def setup_inputs(seed: int = 0, part: int = 0) -> dict:
    streams_of = jax.random.split(jax.random.key(seed), 4)
    part_splits = jax.random.split(jax.random.fold_in(streams_of[3], part), 4)
    return {
        "spectra": normal_values(part_splits[0], (STATIONS, 2, FREQ), 1.0, 6.0, ((0, 128),)),
        "pair_mask": draw_pair_mask(jax.random.fold_in(streams_of[3], 71), part),
        "available": place_ends((jax.random.randint(part_splits[2], (STATIONS,), 0, 8) < 7).astype(jnp.int32), jax.random.fold_in(part_splits[2], 1), 0, 1),
    }


def reference(spectra, pair_mask, available):
    stations = spectra.shape[0]
    freq = spectra.shape[2]
    nfft = 2 * freq
    half = LAGS // 2
    whole = spectra.astype(jnp.float32)
    flags = available.astype(jnp.float32)
    scale = nfft / math.sqrt(8.0 * freq)

    def one_row(item):
        own, mask_row, own_flag = item
        real_part = own[0][None, :] * whole[:, 0, :] + own[1][None, :] * whole[:, 1, :]
        imag_part = own[0][None, :] * whole[:, 1, :] - own[1][None, :] * whole[:, 0, :]
        imag_part = imag_part.at[:, 0].set(0.0)
        nyquist = jnp.zeros((stations, 1), real_part.dtype)
        spectrum = lax.complex(jnp.concatenate([real_part, nyquist], axis=1), jnp.concatenate([imag_part, nyquist], axis=1))
        series = jnp.fft.irfft(spectrum, n=nfft, axis=1)
        lagged = jnp.concatenate([series[:, nfft - half:], series[:, :half]], axis=1) * scale
        return lagged * (mask_row.astype(lagged.dtype) * own_flag * flags)[:, None]
    return lax.map(one_row, (whole, pair_mask, flags))
```

```python
import functools
import math

import jax
import jax.numpy as jnp
import numpy as np
from jax import lax
from jax.experimental import pallas as pl
from jax.experimental.pallas import tpu as pltpu
from jax.sharding import PartitionSpec as P

LAGS = 8192
CORES = 2
ACROSS = 4
INNER = 128


def split_table(table):
    high = table.astype(jnp.bfloat16)
    low = (table - high.astype(np.float64)).astype(jnp.bfloat16)
    return high, low


@functools.cache
def build_tables(freq):
    nfft = 2 * freq
    column = nfft // INNER
    depth = freq // column
    width = column // 2
    outer = LAGS // INNER
    scale = 2.0 / math.sqrt(8.0 * freq)
    lag = np.arange(INNER)[:, None]
    angle = 2.0 * np.pi * ((lag * np.arange(depth)[None, :]) % INNER) / INNER
    after = 2.0 * np.pi * ((lag * (np.arange(depth)[None, :] + 1)) % INNER) / INNER
    section = np.block(
        [
            [np.cos(angle), -np.sin(angle), np.cos(after), -np.sin(after)],
            [np.sin(angle), np.cos(angle), -np.sin(after), -np.cos(after)],
        ]
    )
    first = np.concatenate(split_table(section), axis=0)
    twist = 2.0 * np.pi * ((lag * np.arange(width)[None, :]) % nfft) / nfft
    turn = np.stack([np.cos(twist), np.sin(twist)]).astype(np.float32)
    steps = np.arange(outer)[None, :] - outer // 2
    angle = 2.0 * np.pi * ((np.arange(width)[:, None] * steps) % column) / column
    section = np.concatenate([np.cos(angle), -np.sin(angle)], axis=0) * scale
    second = np.concatenate(split_table(section), axis=1)
    odd = 2 * np.arange(depth)[:, None] + 1
    angle = 2.0 * np.pi * ((odd * lag.T) % (2 * INNER)) / (2 * INNER)
    section = np.concatenate([np.cos(angle), -np.sin(angle)], axis=0) * scale
    middle = np.concatenate(split_table(section), axis=1)
    return first, turn, second, middle


def fold_body(whole_ref, out_ref):
    rows, column = whole_ref.shape
    width = column // 2
    half = rows // 2
    whole = whole_ref[...]
    right = whole[:, width:]
    down = lax.broadcasted_iota(jnp.int32, (width, width), 0)
    over = lax.broadcasted_iota(jnp.int32, (width, width), 1)
    mirror = jnp.where(down == lax.rem(width - over, width), 1.0, 0.0).astype(jnp.bfloat16)
    flipped = jnp.dot(right, mirror, preferred_element_type=jnp.float32).astype(jnp.bfloat16)
    out_ref[pl.ds(0, rows), :] = whole[:, :width]
    out_ref[pl.ds(rows, rows), :] = flipped
    extra = out_ref.shape[0] - 2 * rows
    over = lax.broadcasted_iota(jnp.int32, (extra, width), 1)
    pick = jnp.where(over == 0, 1.0, 0.0).astype(jnp.bfloat16)
    straight = lax.dot_general(
        pick, right, (((1,), (1,)), ((), ())), preferred_element_type=jnp.float32
    )
    crossed = jnp.concatenate([straight[:, half:], -straight[:, :half]], axis=1)
    out_ref[pl.ds(2 * rows, extra), :] = jnp.concatenate([straight, crossed], axis=1).astype(
        jnp.bfloat16
    )


def fold_call(whole):
    rows, column = whole.shape
    return pl.pallas_call(
        fold_body,
        out_shape=jax.ShapeDtypeStruct((2 * rows + 16, column // 2), jnp.bfloat16),
        in_specs=[pl.BlockSpec(memory_space=pltpu.VMEM)],
        out_specs=pl.BlockSpec(memory_space=pltpu.VMEM),
        cost_estimate=pl.CostEstimate(flops=1_000_000, bytes_accessed=300_000, transcendentals=0),
        name="fold",
    )(whole)


def split(value):
    high = value.astype(jnp.bfloat16)
    return high, (value - high.astype(jnp.float32)).astype(jnp.bfloat16)


def cross_spectrum(other, mine):
    parts = []
    quarter = mine.shape[0] // 4
    for n in (0, 2):
        ar, ai = mine[n * quarter : (n + 1) * quarter], mine[(n + 1) * quarter : (n + 2) * quarter]
        br, bi = other[n * quarter : (n + 1) * quarter], other[(n + 1) * quarter : (n + 2) * quarter]
        parts += [ar * br + ai * bi, ar * bi - ai * br]
    return jnp.concatenate(parts, axis=0)


def turned_columns(other, mine, first, turn):
    high, low = split(cross_spectrum(other, mine))
    wide = jnp.dot(first[...], high, preferred_element_type=jnp.float32)
    rest = jnp.dot(first[: 2 * INNER], low, preferred_element_type=jnp.float32)
    mixed = wide[: 2 * INNER] + wide[2 * INNER :] + rest
    sr, si = mixed[:INNER], mixed[INNER:]
    tc, ts = turn[0], turn[1]
    turned = jnp.concatenate([sr * tc - si * ts, sr * ts + si * tc], axis=1)
    return split(turned)


def lags_of(summed, middle):
    summed = summed.T
    outer = summed.shape[0] // 2
    parity = lax.broadcasted_iota(jnp.int32, (outer, INNER), 0) % 2
    return summed[:outer] + summed[outer:] + jnp.where(parity == 0, middle, -middle)


def stage_body(step, plan, along, info, own_w, pair_w, mine0, mine1, first, turn, second, middle, *rest):
    slab_count = sum(present for present, _ in plan)
    slabs, rest = rest[:slab_count], rest[-10:]
    own_hbm, pair_ref, held, wide, mids, kept, result_ref, listed, names, sems = rest
    x, z, c = info[0], info[1], info[2]
    sign = 2 * c - 1
    per = slabs[0].shape[0]
    size = wide.shape[1]
    count = jnp.int32(0)
    taken = 0
    for side, (present, rows) in enumerate(plan):
        if not present:
            continue
        held[pl.ds(side * per, per)] = slabs[taken][...]
        taken += 1
        zj = lax.rem(z + sign * (step - side) + along, along)
        for n in range(per):
            e = side * per + n
            xj = lax.rem(x + side * sign + 2 * (n % 2) + ACROSS, ACROSS)
            j = (xj * along + zj) * CORES + lax.rem(c + n // 2, CORES)
            names[e] = j
            for row in range(rows):
                listed[count] = e * 2 + row
                keep = (own_w if row == 0 else pair_w)[j] != 0.0
                count = count + keep.astype(jnp.int32)

    quarter = size // 4
    down = lax.broadcasted_iota(jnp.int32, wide.shape[1:], 0)
    over = lax.broadcasted_iota(jnp.int32, wide.shape[1:], 1)
    once = (over == 0) & ((down == 0) | (down == quarter))
    weight = jnp.where(once, 0.5, jnp.where((over == 0) & (down >= 2 * quarter), 0.0, 1.0))
    lane = lax.broadcasted_iota(jnp.int32, (2 * per, INNER), 1)
    spot = lax.broadcasted_iota(jnp.int32, (2 * per, INNER), 0)
    straight = jnp.zeros((2 * per, INNER), jnp.float32)
    crossed = jnp.zeros((2 * per, INNER), jnp.float32)
    for side, (present, rows) in enumerate(plan):
        for e in range(side * per, (side + 1) * per if present else 0):
            edge = held[e, size:].astype(jnp.float32)[: 2 * per]
            straight = jnp.where(spot == e, edge[:, :INNER], straight)
            crossed = jnp.where(spot == e, edge[:, INNER:], crossed)
    parts = []
    for row in range(2):
        mine = mine1 if row else mine0
        wide[row] = mine[:size].astype(jnp.float32) * weight
        edge = mine[size:].astype(jnp.float32)[: 2 * per]
        real = jnp.where(lane < INNER // 2, edge[:, :INNER], -edge[:, INNER:])
        imag = jnp.where(lane < INNER // 2, edge[:, INNER:], edge[:, :INNER])
        parts.append(real * straight + imag * crossed)
    high, low = split(jnp.concatenate(parts, axis=0))
    rows_of = high.shape[0]
    summed = jnp.dot(
        jnp.concatenate([high, low], axis=0), middle[...], preferred_element_type=jnp.float32
    )
    summed = summed[:rows_of] + summed[rows_of:]
    mids[...] = summed[:, :INNER] + summed[:, INNER:]

    def copy_out(e):
        return pltpu.make_async_copy(result_ref.at[e], own_hbm.at[names[e]], sems.at[e])

    def compute(code):
        other = held[code // 2, :size].astype(jnp.float32)
        return turned_columns(other, wide[code % 2], first, turn)

    def middle_of(code):
        return mids[pl.ds(lax.rem(code, 2) * 2 * per + code // 2, 1), :]

    def keep_result(code, value):
        e = code // 2

        @pl.when(code % 2 == 0)
        def _():
            result_ref[e] = value
            copy_out(e).start()

        if pair_ref is not None:
            @pl.when(code % 2 != 0)
            def _():
                pair_ref[e] = value

    def two(k, before):
        summed = jnp.dot(kept[...], second[...], preferred_element_type=jnp.float32)
        value0 = lags_of(summed[:INNER] + summed[INNER : 2 * INNER], middle_of(before[0]))
        value1 = lags_of(summed[2 * INNER : 3 * INNER] + summed[3 * INNER :], middle_of(before[1]))
        code0 = listed[jnp.minimum(2 * k, count - 1)]
        code1 = listed[jnp.minimum(2 * k + 1, count - 1)]
        kept[...] = jnp.concatenate([*compute(code0), *compute(code1)], axis=0)

        @pl.when(k > 0)
        def _():
            keep_result(before[0], value0)

        @pl.when((k > 0) & (2 * k - 1 < count))
        def _():
            keep_result(before[1], value1)

        return code0, code1

    trips = jnp.where(count > 0, (count + 1) // 2 + 1, 0)
    lax.fori_loop(0, trips, two, (jnp.int32(0), jnp.int32(0)))
    for side, (present, rows) in enumerate(plan):
        if present:
            for n in range(per):
                e = side * per + n

                @pl.when(own_w[names[e]] != 0.0)
                def _():
                    copy_out(e).wait()


def stage_call(step, plan, along, slabs, info, own_w, pair_w, mine, tables, own_buf, pair_buf, pair_at, pair_size):
    total = own_w.shape[0]
    per = slabs[0].shape[0]
    count = 2 * per
    outer = LAGS // INNER
    smem = pl.BlockSpec(memory_space=pltpu.SMEM)
    vmem = pl.BlockSpec(memory_space=pltpu.VMEM)
    hbm = pl.BlockSpec(memory_space=pl.ANY)
    args = [info, own_w, pair_w, *mine, *tables, *slabs]
    specs = [smem] * 3 + [vmem] * (2 + len(tables) + len(slabs))
    out_shape = [jax.ShapeDtypeStruct((total, outer, INNER), jnp.float32)]
    out_specs = [hbm]
    aliases = {}
    if own_buf is not None:
        aliases[len(args)] = 0
        args.append(own_buf)
        specs.append(hbm)
    with_pair = pair_size is not None
    if with_pair:
        out_shape.append(jax.ShapeDtypeStruct((pair_size, outer, INNER), jnp.float32))
        out_specs.append(pl.BlockSpec((count, outer, INNER), lambda g: (pair_at, 0, 0)))
        if pair_buf is not None:
            aliases[len(args)] = 1
            args.append(pair_buf)
            specs.append(hbm)

    def body(*refs):
        scratch = refs[-8:]
        outs = refs[len(args) : -8]
        pair_ref = outs[1] if with_pair else None
        stage_body(
            step, plan, along, *refs[: 5 + len(tables) + len(slabs)], outs[0], pair_ref, *scratch
        )

    flops = sum(rows * per for present, rows in plan if present) * 100_000_000
    return pl.pallas_call(
        body,
        grid=(1,),
        out_shape=out_shape,
        in_specs=specs,
        out_specs=out_specs,
        scratch_shapes=[
            pltpu.VMEM((count,) + mine[0].shape, jnp.bfloat16),
            pltpu.VMEM((2, 2 * INNER, mine[0].shape[1]), jnp.float32),
            pltpu.VMEM((2 * count, INNER), jnp.float32),
            pltpu.VMEM((4 * INNER, 2 * mine[0].shape[1]), jnp.bfloat16),
            pltpu.VMEM((count, outer, INNER), jnp.float32),
            pltpu.SMEM((2 * count + 1,), jnp.int32),
            pltpu.SMEM((count,), jnp.int32),
            pltpu.SemaphoreType.DMA((count,)),
        ],
        input_output_aliases=aliases,
        cost_estimate=pl.CostEstimate(flops=flops, bytes_accessed=3_000_000, transcendentals=0),
        name=f"stage{step}",
    )(*args)


def finish_body(src_ref, own_w, own_ref, early_ref, late_ref, out_ref, lines):
    g = pl.program_id(0)
    first = early_ref.shape[0]
    outer = own_ref.shape[1]
    pitch = outer + 8
    for k in range(8):
        src = src_ref[g * 8 + k]
        live = own_w[g * 8 + k] != 0.0
        early = early_ref[jnp.clip(src, 0, first - 1)]
        late = late_ref[jnp.clip(src - first, 0, late_ref.shape[0] - 1)]
        value = jnp.where(src < 0, own_ref[k], jnp.where(src < first, early, late))
        lines[pl.ds(k * pitch, outer), :] = jnp.where(live, value, 0.0)
    for n in range(outer):
        out_ref[pl.ds(8 * n, 8), :] = lines[pl.ds(n, 8, stride=pitch), :]


def finish_call(src, own_w, own_buf, early, late):
    outer = LAGS // INNER
    total = src.shape[0]
    smem = pl.BlockSpec(memory_space=pltpu.SMEM)
    vmem = pl.BlockSpec(memory_space=pltpu.VMEM)
    return pl.pallas_call(
        finish_body,
        grid=(total // 8,),
        out_shape=jax.ShapeDtypeStruct((total * outer, INNER), jnp.float32),
        in_specs=[smem, smem, pl.BlockSpec((8, outer, INNER), lambda g: (g, 0, 0)), vmem, vmem],
        out_specs=pl.BlockSpec((8 * outer, INNER), lambda g: (g, 0)),
        scratch_shapes=[pltpu.VMEM((8 * (outer + 8), INNER), jnp.float32)],
        cost_estimate=pl.CostEstimate(flops=1_000_000, bytes_accessed=8_000_000, transcendentals=0),
        name="finish",
    )(src, own_w, own_buf, early, late)


def per_device(total, spectra, pair_mask, available):
    along = total // (ACROSS * CORES)
    far = along // 2
    freq = spectra.shape[2]
    column = 2 * freq // INNER
    tables = [jnp.asarray(table) for table in build_tables(freq)]

    def move(value, goal_of):
        pairs = []
        for start in range(total):
            x, z, c = start // (along * CORES), start // CORES % along, start % CORES
            x, z, c = goal_of(x, z, c)
            pairs.append((start, (x % ACROSS * along + z % along) * CORES + c % CORES))
        return lax.ppermute(value, "row", pairs)

    def swap(value):
        return move(value, lambda x, z, c: (x, z, c + 1))

    def onward(value):
        return move(value, lambda x, z, c: (x, z + 1 - 2 * c, c))

    def sideways(value):
        return move(value, lambda x, z, c: (x + 1 - 2 * c, z, c))

    me = lax.axis_index("row")
    x, z, c = me // (along * CORES), me // CORES % along, me % CORES
    info = jnp.stack([x, z, c]).astype(jnp.int32)

    own = fold_call(spectra.reshape(2 * freq // column, column))
    across = move(own, lambda x, z, c: (x + 2 - 4 * c, z, c))
    flag = lax.dynamic_slice_in_dim(available, me, 1, 0).astype(jnp.float32)
    own_w = pair_mask[0].astype(jnp.float32) * flag * available.astype(jnp.float32)
    pair_w = swap(own_w)
    other = swap(own)
    across, pair_w, other, info = lax.optimization_barrier((across, pair_w, other, info))
    slab = jnp.stack([own, across, other, swap(across)])
    mine = (own, other)

    cut = far - 2
    early = late = own_buf = side = None
    for step in range(far + 2):
        plan, slabs = [], []
        for value, stage in ((slab, step), (side, step - 1)):
            plan.append((value is not None, 2 if 0 < stage < far else 1))
            if value is not None:
                slabs.append(value)
        next_slab = onward(slab) if step < far else None
        side = sideways(slab) if step <= far else None
        paired = 1 <= step <= far
        if paired and step <= cut:
            buf, at, size = early, step - 1, 8 * cut
        elif paired:
            buf, at, size = late, step - 1 - cut, 8 * (far - cut)
        else:
            buf, at, size = None, None, None
        outs = stage_call(
            step, plan, along, slabs, info, own_w, pair_w, mine, tables, own_buf, buf, at, size
        )
        own_buf = outs[0]
        if paired and step <= cut:
            early = outs[1]
        elif paired:
            late = outs[1]
        slab = next_slab
        if step <= far:
            slab, side, own_buf, early, late = lax.optimization_barrier(
                (slab, side, own_buf, early, late)
            )
    early, late = swap(early), swap(late)

    j = lax.iota(jnp.int32, total)
    xj, zj, cj = j // (along * CORES), j // CORES % along, j % CORES
    dx, dz = (xj - x) % ACROSS, (zj - z) % along
    host = (dz < far).astype(jnp.int32)
    stage = jnp.where(dz < far, dz, along - dz)
    beside = dx % 2
    half = jnp.where(beside == 1, (dx + 1 - 2 * host) % ACROSS // 2, dx // 2)
    entry = 4 * beside + 2 * ((cj - host) % CORES) + half
    far_one = (host != c) & (dz != 0) & (dz != far)
    src = jnp.where(far_one, 8 * (stage - 1 + beside) + entry, -1).astype(jnp.int32)
    out = finish_call(src, own_w, own_buf, early, late)
    out = out.reshape(total // 8, LAGS // INNER, 8, INNER)
    return jnp.transpose(out, (0, 2, 1, 3)).reshape(1, total, LAGS)


def solution(mesh):
    return jax.shard_map(
        functools.partial(per_device, mesh.shape["row"]),
        mesh=mesh,
        in_specs=(P(("win", "row"), None, None), P("row", None), P("win")),
        out_specs=P(("win", "row"), None, None),
        check_vma=False,
    )
```

```python
import functools
import math

import jax
import jax.numpy as jnp
import numpy as np
from jax import lax
from jax.experimental import pallas as pl
from jax.experimental.pallas import tpu as pltpu
from jax.sharding import PartitionSpec as P


LAGS = 8192
CORES = 2
ACROSS = 4
INNER = 128


def split_table(table):
    high = table.astype(jnp.bfloat16)
    low = (table - high.astype(np.float64)).astype(jnp.bfloat16)
    return high, low


@functools.cache
def build_tables(freq):
    nfft = 2 * freq
    column = nfft // INNER
    depth = freq // column
    width = column // 2
    outer = LAGS // INNER
    scale = 2.0 / math.sqrt(8.0 * freq)
    lag = np.arange(INNER)[:, None]
    angle = 2.0 * np.pi * ((lag * np.arange(depth)[None, :]) % INNER) / INNER
    after = 2.0 * np.pi * ((lag * (np.arange(depth)[None, :] + 1)) % INNER) / INNER
    section = np.block(
        [
            [np.cos(angle), -np.sin(angle), np.cos(after), -np.sin(after)],
            [np.sin(angle), np.cos(angle), -np.sin(after), -np.cos(after)],
        ]
    )
    first = np.concatenate(split_table(section), axis=0)
    twist = 2.0 * np.pi * ((lag * np.arange(width)[None, :]) % nfft) / nfft
    turn = np.stack([np.cos(twist), np.sin(twist)]).astype(np.float32)
    steps = np.arange(outer)[None, :] - outer // 2
    angle = 2.0 * np.pi * ((np.arange(width)[:, None] * steps) % column) / column
    section = np.concatenate([np.cos(angle), -np.sin(angle)], axis=0) * scale
    second = np.concatenate(split_table(section), axis=1)
    odd = 2 * np.arange(depth)[:, None] + 1
    angle = 2.0 * np.pi * ((odd * lag.T) % (2 * INNER)) / (2 * INNER)
    section = np.concatenate([np.cos(angle), -np.sin(angle)], axis=0) * scale
    middle = np.concatenate(split_table(section), axis=1)
    return first, turn, second, middle


def fold_body(whole_ref, *refs):
    many = (len(refs) - 2) // 2
    sources, out_ref, copied, sems = refs[:many], refs[many], refs[many + 1 : -1], refs[-1]
    copies = [
        pltpu.make_async_copy(source, target, sems.at[n])
        for n, (source, target) in enumerate(zip(sources, copied))
    ]
    for copy in copies:
        copy.start()
    rows, column = whole_ref.shape
    width = column // 2
    half = rows // 2
    whole = whole_ref[...]
    right = whole[:, width:]
    down = lax.broadcasted_iota(jnp.int32, (width, width), 0)
    over = lax.broadcasted_iota(jnp.int32, (width, width), 1)
    mirror = jnp.where(down == lax.rem(width - over, width), 1.0, 0.0).astype(jnp.bfloat16)
    flipped = jnp.dot(right, mirror, preferred_element_type=jnp.float32).astype(jnp.bfloat16)
    out_ref[pl.ds(0, rows), :] = whole[:, :width]
    out_ref[pl.ds(rows, rows), :] = flipped
    extra = out_ref.shape[0] - 2 * rows
    over = lax.broadcasted_iota(jnp.int32, (extra, width), 1)
    pick = jnp.where(over == 0, 1.0, 0.0).astype(jnp.bfloat16)
    straight = lax.dot_general(
        pick, right, (((1,), (1,)), ((), ())), preferred_element_type=jnp.float32
    )
    crossed = jnp.concatenate([straight[:, half:], -straight[:, :half]], axis=1)
    out_ref[pl.ds(2 * rows, extra), :] = jnp.concatenate([straight, crossed], axis=1).astype(
        jnp.bfloat16
    )
    for copy in copies:
        copy.wait()


def fold_call(whole, tables):
    rows, column = whole.shape
    vmem = pl.BlockSpec(memory_space=pltpu.VMEM)
    hbm = pl.BlockSpec(memory_space=pltpu.HBM)
    own = jax.ShapeDtypeStruct((2 * rows + 16, column // 2), jnp.bfloat16)
    return pl.pallas_call(
        fold_body,
        out_shape=[own] + [jax.ShapeDtypeStruct(table.shape, table.dtype) for table in tables],
        in_specs=[vmem] + [hbm] * len(tables),
        out_specs=[vmem] * (1 + len(tables)),
        scratch_shapes=[pltpu.SemaphoreType.DMA((len(tables),))],
        cost_estimate=pl.CostEstimate(flops=1_000_000, bytes_accessed=300_000, transcendentals=0),
        compiler_params=pltpu.CompilerParams(vmem_limit_bytes=16 * 1024 * 1024),
        name="fold",
    )(whole, *tables)


def split(value):
    high = value.astype(jnp.bfloat16)
    return high, (value - high.astype(jnp.float32)).astype(jnp.bfloat16)


def cross_spectrum(other, mine):
    parts = []
    quarter = mine.shape[0] // 4
    for n in (0, 2):
        ar, ai = mine[n * quarter : (n + 1) * quarter], mine[(n + 1) * quarter : (n + 2) * quarter]
        br, bi = other[n * quarter : (n + 1) * quarter], other[(n + 1) * quarter : (n + 2) * quarter]
        parts += [ar * br + ai * bi, ar * bi - ai * br]
    return jnp.concatenate(parts, axis=0)


def turned_columns(high, low, first, turn):
    wide = jnp.dot(first[...], high, preferred_element_type=jnp.float32)
    rest = jnp.dot(first[: 2 * INNER], low, preferred_element_type=jnp.float32)
    mixed = wide[: 2 * INNER] + wide[2 * INNER :] + rest
    sr, si = mixed[:INNER], mixed[INNER:]
    tc, ts = turn[0], turn[1]
    turned = jnp.concatenate([sr * tc - si * ts, sr * ts + si * tc], axis=1)
    return split(turned)


def lags_of(summed, middle):
    summed = summed.T
    outer = summed.shape[0] // 2
    parity = lax.broadcasted_iota(jnp.int32, (outer, INNER), 0) % 2
    return summed[:outer] + summed[outer:] + jnp.where(parity == 0, middle, -middle)


def stage_body(step, plan, along, pair_at, info, own_w, pair_w, mine0, mine1, first, turn, second, middle, *rest):
    chains = 2
    slab_count = chains * sum(present for present, _ in plan)
    slabs, rest = rest[:slab_count], rest[-12:]
    own_hbm, pair_hbm, token, held, wide, mids, ahead, kept, result_ref, listed, names, sems = rest
    token[...] = jnp.zeros_like(token)
    x, z, c = info[0], info[1], info[2]
    sign = 2 * c - 1
    part = slabs[0].shape[0]
    per = chains * part
    size = wide.shape[1]
    count = jnp.int32(0)
    taken = 0
    for side, (present, rows) in enumerate(plan):
        if not present:
            continue
        for chain in range(chains):
            held[pl.ds(side * per + chain * part, part)] = slabs[taken][...]
            taken += 1
        zj = lax.rem(z + sign * (step - side) + along, along)
        for n in range(per):
            e = side * per + n
            xj = lax.rem(x + side * sign + 2 * (n % 2) + ACROSS, ACROSS)
            j = (xj * along + zj) * CORES + lax.rem(c + n // 2, CORES)
            names[e] = j
            for row in range(rows):
                listed[count] = e * 2 + row
                keep = (own_w if row == 0 else pair_w)[j] != 0.0
                count = count + keep.astype(jnp.int32)

    quarter = size // 4
    down = lax.broadcasted_iota(jnp.int32, wide.shape[1:], 0)
    over = lax.broadcasted_iota(jnp.int32, wide.shape[1:], 1)
    once = (over == 0) & ((down == 0) | (down == quarter))
    weight = jnp.where(once, 0.5, jnp.where((over == 0) & (down >= 2 * quarter), 0.0, 1.0))
    lane = lax.broadcasted_iota(jnp.int32, (2 * per, INNER), 1)
    spot = lax.broadcasted_iota(jnp.int32, (2 * per, INNER), 0)
    straight = jnp.zeros((2 * per, INNER), jnp.float32)
    crossed = jnp.zeros((2 * per, INNER), jnp.float32)
    for side, (present, rows) in enumerate(plan):
        for e in range(side * per, (side + 1) * per if present else 0):
            edge = held[e, size:].astype(jnp.float32)[: 2 * per]
            straight = jnp.where(spot == e, edge[:, :INNER], straight)
            crossed = jnp.where(spot == e, edge[:, INNER:], crossed)
    parts = []
    for row in range(2):
        mine = mine1 if row else mine0
        wide[row] = mine[:size].astype(jnp.float32) * weight
        edge = mine[size:].astype(jnp.float32)[: 2 * per]
        real = jnp.where(lane < INNER // 2, edge[:, :INNER], -edge[:, INNER:])
        imag = jnp.where(lane < INNER // 2, edge[:, INNER:], edge[:, :INNER])
        parts.append(real * straight + imag * crossed)
    high, low = split(jnp.concatenate(parts, axis=0))
    rows_of = high.shape[0]
    summed = jnp.dot(
        jnp.concatenate([high, low], axis=0), middle[...], preferred_element_type=jnp.float32
    )
    summed = summed[:rows_of] + summed[rows_of:]
    mids[...] = summed[:, :INNER] + summed[:, INNER:]

    def copy_out(code):
        e = code // 2
        return pltpu.make_async_copy(result_ref.at[code], own_hbm.at[names[e]], sems.at[code])

    def copy_pair(code):
        to = pair_hbm.at[pair_at + code // 2]
        return pltpu.make_async_copy(result_ref.at[code], to, sems.at[code])

    def spectrum(code):
        return split(cross_spectrum(held[code // 2, :size].astype(jnp.float32), wide[code % 2]))

    def columns(n):
        return turned_columns(ahead[2 * n], ahead[2 * n + 1], first, turn)

    def middle_of(code):
        return mids[pl.ds(lax.rem(code, 2) * 2 * per + code // 2, 1), :]

    def keep_result(code, value):
        result_ref[code] = value

        @pl.when(code % 2 == 0)
        def _():
            copy_out(code).start()

        if pair_hbm is not None:
            @pl.when(code % 2 != 0)
            def _():
                copy_pair(code).start()

    def two(k, before):
        done0, done1 = before[:2]
        summed = jnp.dot(kept[...], second[...], preferred_element_type=jnp.float32)
        value0 = lags_of(summed[:INNER] + summed[INNER : 2 * INNER], middle_of(done0))
        value1 = lags_of(summed[2 * INNER : 3 * INNER] + summed[3 * INNER :], middle_of(done1))
        kept[...] = jnp.concatenate([*columns(0), *columns(1)], axis=0)
        code0 = listed[jnp.minimum(2 * k, count - 1)]
        code1 = listed[jnp.minimum(2 * k + 1, count - 1)]
        for n, code in enumerate((code0, code1)):
            ahead[2 * n], ahead[2 * n + 1] = spectrum(code)

        @pl.when(k > 1)
        def _():
            keep_result(done0, value0)

        @pl.when((k > 1) & (2 * k - 3 < count))
        def _():
            keep_result(done1, value1)

        return *before[2:], code0, code1

    trips = jnp.where(count > 0, (count + 1) // 2 + 2, 0)
    lax.fori_loop(0, trips, two, (jnp.int32(0),) * 4)
    for side, (present, rows) in enumerate(plan):
        for e in range(side * per, (side + 1) * per if present else 0):
            @pl.when(own_w[names[e]] != 0.0)
            def _():
                copy_out(2 * e).wait()

            if rows > 1:
                @pl.when(pair_w[names[e]] != 0.0)
                def _():
                    copy_pair(2 * e + 1).wait()


def stage_call(step, plan, along, slabs, info, own_w, pair_w, mine, tables, own_buf, pair_buf, pair_at, pair_size):
    total = own_w.shape[0]
    count = 4 * slabs[0].shape[0]
    outer = LAGS // INNER
    smem = pl.BlockSpec(memory_space=pltpu.SMEM)
    vmem = pl.BlockSpec(memory_space=pltpu.VMEM)
    hbm = pl.BlockSpec(memory_space=pl.ANY)
    args = [info, own_w, pair_w, *mine, *tables, *slabs]
    specs = [smem] * 3 + [vmem] * (2 + len(tables) + len(slabs))
    used = len(args)
    out_shape = [jax.ShapeDtypeStruct((8, INNER), jnp.float32)]
    out_shape.append(jax.ShapeDtypeStruct((total, outer, INNER), jnp.float32))
    out_specs = [vmem, hbm]
    aliases = {}
    if own_buf is not None:
        aliases[len(args)] = 1
        args.append(own_buf)
        specs.append(hbm)
    with_pair = pair_size is not None
    if with_pair:
        out_shape.append(jax.ShapeDtypeStruct((pair_size, outer, INNER), jnp.float32))
        out_specs.append(hbm)
        if pair_buf is not None:
            aliases[len(args)] = 2
            args.append(pair_buf)
            specs.append(hbm)

    def body(*refs):
        scratch = refs[-9:]
        outs = refs[len(args) : -9]
        pair_ref = outs[2] if with_pair else None
        stage_body(step, plan, along, pair_at, *refs[:used], outs[1], pair_ref, outs[0], *scratch)

    flops = sum(rows * count // 2 for present, rows in plan if present) * 100_000_000
    return pl.pallas_call(
        body,
        out_shape=out_shape,
        in_specs=specs,
        out_specs=out_specs,
        scratch_shapes=[
            pltpu.VMEM((count,) + mine[0].shape, jnp.bfloat16),
            pltpu.VMEM((2, 2 * INNER, mine[0].shape[1]), jnp.float32),
            pltpu.VMEM((2 * count, INNER), jnp.float32),
            pltpu.VMEM((4, 2 * INNER, mine[0].shape[1]), jnp.bfloat16),
            pltpu.VMEM((4 * INNER, 2 * mine[0].shape[1]), jnp.bfloat16),
            pltpu.VMEM((2 * count, outer, INNER), jnp.float32),
            pltpu.SMEM((2 * count + 1,), jnp.int32),
            pltpu.SMEM((count,), jnp.int32),
            pltpu.SemaphoreType.DMA((2 * count,)),
        ],
        input_output_aliases=aliases,
        cost_estimate=pl.CostEstimate(flops=flops, bytes_accessed=3_000_000, transcendentals=0),
        compiler_params=pltpu.CompilerParams(vmem_limit_bytes=16 * 1024 * 1024),
    )(*args)


def finish_body(src_ref, own_w, own_ref, early_ref, late_ref, out_ref, lines):
    g = pl.program_id(0)
    first = early_ref.shape[0]
    block, outer = own_ref.shape[:2]
    pitch = outer + 8

    def tile(m, _):
        for k in range(8):
            j = g * block + m * 8 + k
            src = src_ref[j]
            live = own_w[j] != 0.0
            early = early_ref[jnp.clip(src, 0, first - 1)]
            late = late_ref[jnp.clip(src - first, 0, late_ref.shape[0] - 1)]
            value = jnp.where(src < 0, own_ref[m * 8 + k], jnp.where(src < first, early, late))
            lines[pl.ds(k * pitch, outer), :] = jnp.where(live, value, 0.0)
        for n in range(outer):
            to = pl.ds(pl.multiple_of(m * 8 * outer + 8 * n, 8), 8)
            out_ref[to, :] = lines[pl.ds(n, 8, stride=pitch), :]
        return 0

    lax.fori_loop(0, block // 8, tile, 0)


def finish_call(src, own_w, own_buf, early, late):
    outer = LAGS // INNER
    total = src.shape[0]
    block = 32
    smem = pl.BlockSpec(memory_space=pltpu.SMEM)
    vmem = pl.BlockSpec(memory_space=pltpu.VMEM)
    return pl.pallas_call(
        finish_body,
        grid=(total // block,),
        out_shape=jax.ShapeDtypeStruct((total * outer, INNER), jnp.float32),
        in_specs=[smem, smem, pl.BlockSpec((block, outer, INNER), lambda g: (g, 0, 0)), vmem, vmem],
        out_specs=pl.BlockSpec((block * outer, INNER), lambda g: (g, 0)),
        scratch_shapes=[pltpu.VMEM((8 * (outer + 8), INNER), jnp.float32)],
        cost_estimate=pl.CostEstimate(flops=1_000_000, bytes_accessed=8_000_000, transcendentals=0),
        compiler_params=pltpu.CompilerParams(vmem_limit_bytes=16 * 1024 * 1024),
        name="finish",
    )(src, own_w, own_buf, early, late)


def per_device(total, spectra, pair_mask, available):
    along = total // (ACROSS * CORES)
    far = along // 2
    freq = spectra.shape[2]
    column = 2 * freq // INNER
    tables = [jnp.asarray(table) for table in build_tables(freq)]

    def move(value, goal_of):
        pairs = []
        for start in range(total):
            x, z, c = start // (along * CORES), start // CORES % along, start % CORES
            x, z, c = goal_of(x, z, c)
            pairs.append((start, (x % ACROSS * along + z % along) * CORES + c % CORES))
        return lax.ppermute(value, "row", pairs)

    def swap(value):
        return move(value, lambda x, z, c: (x, z, c + 1))

    def onward(value):
        return move(value, lambda x, z, c: (x, z + 1 - 2 * c, c))

    def sideways(value):
        return move(value, lambda x, z, c: (x + 1 - 2 * c, z, c))

    me = lax.axis_index("row")
    x, z, c = me // (along * CORES), me // CORES % along, me % CORES
    info = jnp.stack([x, z, c]).astype(jnp.int32)

    own, *tables = fold_call(spectra.reshape(2 * freq // column, column), tables)
    across = move(own, lambda x, z, c: (x + 2 - 4 * c, z, c))
    flag = lax.dynamic_slice_in_dim(available, me, 1, 0).astype(jnp.float32)
    own_w = pair_mask[0].astype(jnp.float32) * flag * available.astype(jnp.float32)
    pair_w = swap(own_w)
    other = swap(own)
    across, pair_w, other, info = lax.optimization_barrier((across, pair_w, other, info))
    slab = (jnp.stack([own, across]), jnp.stack([other, swap(across)]))
    mine = (own, other)

    cut = far - 2
    early = late = own_buf = side = None
    for step in range(far + 2):
        plan, slabs = [], []
        for value, stage in ((slab, step), (side, step - 1)):
            plan.append((value is not None, 2 if 0 < stage < far else 1))
            slabs += value or ()
        next_slab, beside = [], []
        for part in slab or ():
            if step < far:
                next_slab.append(onward(part))
        for part in slab or ():
            beside.append(sideways(part))
        side = tuple(beside) or None
        next_slab = tuple(next_slab) or None
        paired = 1 <= step <= far
        if paired and step <= cut:
            buf, at, size = early, 8 * (step - 1), 8 * cut
        elif paired:
            buf, at, size = late, 8 * (step - 1 - cut), 8 * (far - cut)
        else:
            buf, at, size = None, None, None
        token, own_buf, *pair_buf = stage_call(
            step, plan, along, slabs, info, own_w, pair_w, mine, tables, own_buf, buf, at, size
        )
        if paired and step <= cut:
            early = pair_buf[0]
        elif paired:
            late = pair_buf[0]

        def after(parts):
            return parts and tuple(lax.optimization_barrier((part, token))[0] for part in parts)

        slab, side = after(next_slab), side if step > far else after(side)
    early, late = swap(early), swap(late)

    j = lax.iota(jnp.int32, total)
    xj, zj, cj = j // (along * CORES), j // CORES % along, j % CORES
    dx, dz = (xj - x) % ACROSS, (zj - z) % along
    host = (dz < far).astype(jnp.int32)
    stage = jnp.where(dz < far, dz, along - dz)
    beside = dx % 2
    half = jnp.where(beside == 1, (dx + 1 - 2 * host) % ACROSS // 2, dx // 2)
    entry = 4 * beside + 2 * ((cj - host) % CORES) + half
    far_one = (host != c) & (dz != 0) & (dz != far)
    src = jnp.where(far_one, 8 * (stage - 1 + beside) + entry, -1).astype(jnp.int32)
    out = finish_call(src, own_w, own_buf, early, late)
    out = out.reshape(total // 8, LAGS // INNER, 8, INNER)
    return jnp.transpose(out, (0, 2, 1, 3)).reshape(1, total, LAGS)


def solution(mesh):
    total = mesh.shape["row"]

    def program(*args):
        return per_device(total, *args)

    return jax.shard_map(
        program,
        mesh=mesh,
        in_specs=(P(("win", "row"), None, None), P("row", None), P("win")),
        out_specs=P(("win", "row"), None, None),
        check_vma=False,
    )
```

```python
import functools
import math

import jax
import jax.numpy as jnp
import numpy as np
from jax import lax
from jax.experimental import pallas as pl
from jax.experimental.pallas import tpu as pltpu
from jax.sharding import PartitionSpec as P


LAGS = 8192
CORES = 2
ACROSS = 4
INNER = 128
CHAINS = 1


def split_table(table):
    high = table.astype(jnp.bfloat16)
    low = (table - high.astype(np.float64)).astype(jnp.bfloat16)
    return high, low


@functools.cache
def build_tables(freq):
    nfft = 2 * freq
    column = nfft // INNER
    depth = freq // column
    width = column // 2
    outer = LAGS // INNER
    scale = 2.0 / math.sqrt(8.0 * freq)
    lag = np.arange(INNER)[:, None]
    angle = 2.0 * np.pi * ((lag * np.arange(depth)[None, :]) % INNER) / INNER
    after = 2.0 * np.pi * ((lag * (np.arange(depth)[None, :] + 1)) % INNER) / INNER
    section = np.block(
        [
            [np.cos(angle), -np.sin(angle), np.cos(after), -np.sin(after)],
            [np.sin(angle), np.cos(angle), -np.sin(after), -np.cos(after)],
        ]
    )
    first = np.concatenate(split_table(section), axis=0)
    twist = 2.0 * np.pi * ((lag * np.arange(width)[None, :]) % nfft) / nfft
    turn = np.stack([np.cos(twist), np.sin(twist)]).astype(np.float32)
    steps = np.arange(outer)[None, :] - outer // 2
    angle = 2.0 * np.pi * ((np.arange(width)[:, None] * steps) % column) / column
    section = np.concatenate([np.cos(angle), -np.sin(angle)], axis=0) * scale
    second = np.concatenate(split_table(section), axis=1)
    odd = 2 * np.arange(depth)[:, None] + 1
    angle = 2.0 * np.pi * ((odd * lag.T) % (2 * INNER)) / (2 * INNER)
    section = np.concatenate([np.cos(angle), -np.sin(angle)], axis=0) * scale
    middle = np.concatenate(split_table(section), axis=1)
    wide = np.concatenate([second[:width], second[width:]], axis=1)
    return np.concatenate([first, wide, middle], axis=0), turn


def fold_body(whole_ref, *refs):
    many = (len(refs) - 2) // 2
    sources, out_ref, copied, sems = refs[:many], refs[many], refs[many + 1 : -1], refs[-1]
    copies = [
        pltpu.make_async_copy(source, target, sems.at[n])
        for n, (source, target) in enumerate(zip(sources, copied))
    ]
    for copy in copies:
        copy.start()
    rows, column = whole_ref.shape
    width = column // 2
    half = rows // 2
    whole = whole_ref[...]
    right = whole[:, width:]
    down = lax.broadcasted_iota(jnp.int32, (width, width), 0)
    over = lax.broadcasted_iota(jnp.int32, (width, width), 1)
    mirror = jnp.where(down == lax.rem(width - over, width), 1.0, 0.0).astype(jnp.bfloat16)
    flipped = jnp.dot(right, mirror, preferred_element_type=jnp.float32).astype(jnp.bfloat16)
    out_ref[pl.ds(0, rows), :] = whole[:, :width]
    out_ref[pl.ds(rows, rows), :] = flipped
    extra = out_ref.shape[0] - 2 * rows
    over = lax.broadcasted_iota(jnp.int32, (extra, width), 1)
    pick = jnp.where(over == 0, 1.0, 0.0).astype(jnp.bfloat16)
    straight = lax.dot_general(
        pick, right, (((1,), (1,)), ((), ())), preferred_element_type=jnp.float32
    )
    crossed = jnp.concatenate([straight[:, half:], -straight[:, :half]], axis=1)
    out_ref[pl.ds(2 * rows, extra), :] = jnp.concatenate([straight, crossed], axis=1).astype(
        jnp.bfloat16
    )
    for copy in copies:
        copy.wait()


def fold_call(whole, tables):
    rows, column = whole.shape
    vmem = pl.BlockSpec(memory_space=pltpu.VMEM)
    hbm = pl.BlockSpec(memory_space=pltpu.HBM)
    own = jax.ShapeDtypeStruct((2 * rows + 16, column // 2), jnp.bfloat16)
    return pl.pallas_call(
        fold_body,
        out_shape=[own] + [jax.ShapeDtypeStruct(table.shape, table.dtype) for table in tables],
        in_specs=[vmem] + [hbm] * len(tables),
        out_specs=[vmem] * (1 + len(tables)),
        scratch_shapes=[pltpu.SemaphoreType.DMA((len(tables),))],
        cost_estimate=pl.CostEstimate(flops=1_000_000, bytes_accessed=300_000, transcendentals=0),
        compiler_params=pltpu.CompilerParams(vmem_limit_bytes=16 * 1024 * 1024),
        name="fold",
    )(whole, *tables)


def split(value):
    high = value.astype(jnp.bfloat16)
    return high, (value - high.astype(jnp.float32)).astype(jnp.bfloat16)


def cross_spectrum(other, mine):
    parts = []
    quarter = mine.shape[0] // 4
    for n in (0, 2):
        ar, ai = mine[n * quarter : (n + 1) * quarter], mine[(n + 1) * quarter : (n + 2) * quarter]
        br, bi = other[n * quarter : (n + 1) * quarter], other[(n + 1) * quarter : (n + 2) * quarter]
        parts += [ar * br + ai * bi, ar * bi - ai * br]
    return jnp.concatenate(parts, axis=0)


def turned_columns(high, low, table, turn):
    wide = jnp.dot(table[: 4 * INNER], high, preferred_element_type=jnp.float32)
    rest = jnp.dot(table[: 2 * INNER], low, preferred_element_type=jnp.float32)
    mixed = wide[: 2 * INNER] + wide[2 * INNER :] + rest
    sr, si = mixed[:INNER], mixed[INNER:]
    tc, ts = turn[0], turn[1]
    turned = jnp.concatenate([sr * tc - si * ts, sr * ts + si * tc], axis=1)
    return split(turned)


def lags_of(summed, middle):
    summed = summed.T
    outer = summed.shape[0] // 2
    parity = lax.broadcasted_iota(jnp.int32, (outer, INNER), 0) % 2
    return summed[:outer] + summed[outer:] + jnp.where(parity == 0, middle, -middle)


def stage_body(step, plan, along, pair_at, info, own_w, pair_w, mine0, mine1, table, turn, *rest):
    chains = CHAINS
    slab_count = chains * sum(present for present, _ in plan)
    slabs, rest = rest[:slab_count], rest[-11:]
    own_hbm, pair_hbm, token, held, wide, mids, kept, result_ref, listed, names, sems = rest
    token[...] = jnp.zeros_like(token)
    x, z, c = info[0], info[1], info[2]
    sign = 2 * c - 1
    part = slabs[0].shape[0]
    per = chains * part
    size = wide.shape[1]
    count = jnp.int32(0)
    taken = 0
    for side, (present, rows) in enumerate(plan):
        if not present:
            continue
        for chain in range(chains):
            held[pl.ds(side * per + chain * part, part)] = slabs[taken][...]
            taken += 1
        zj = lax.rem(z + sign * (step - side) + along, along)
        for n in range(per):
            e = side * per + n
            xj = lax.rem(x + side * sign + 2 * (n % 2) + ACROSS, ACROSS)
            j = (xj * along + zj) * CORES + lax.rem(c + n // 2, CORES)
            names[e] = j
            for row in range(rows):
                listed[count] = e * 2 + row
                keep = (own_w if row == 0 else pair_w)[j] != 0.0
                count = count + keep.astype(jnp.int32)

    quarter = size // 4
    down = lax.broadcasted_iota(jnp.int32, wide.shape[1:], 0)
    over = lax.broadcasted_iota(jnp.int32, wide.shape[1:], 1)
    once = (over == 0) & ((down == 0) | (down == quarter))
    weight = jnp.where(once, 0.5, jnp.where((over == 0) & (down >= 2 * quarter), 0.0, 1.0))
    lane = lax.broadcasted_iota(jnp.int32, (2 * per, INNER), 1)
    spot = lax.broadcasted_iota(jnp.int32, (2 * per, INNER), 0)
    straight = jnp.zeros((2 * per, INNER), jnp.float32)
    crossed = jnp.zeros((2 * per, INNER), jnp.float32)
    for side, (present, rows) in enumerate(plan):
        for e in range(side * per, (side + 1) * per if present else 0):
            edge = held[e, size:].astype(jnp.float32)[: 2 * per]
            straight = jnp.where(spot == e, edge[:, :INNER], straight)
            crossed = jnp.where(spot == e, edge[:, INNER:], crossed)
    parts = []
    for row in range(2):
        mine = mine1 if row else mine0
        wide[row] = mine[:size].astype(jnp.float32) * weight
        edge = mine[size:].astype(jnp.float32)[: 2 * per]
        real = jnp.where(lane < INNER // 2, edge[:, :INNER], -edge[:, INNER:])
        imag = jnp.where(lane < INNER // 2, edge[:, INNER:], edge[:, :INNER])
        parts.append(real * straight + imag * crossed)
    high, low = split(jnp.concatenate(parts, axis=0))
    rows_of = high.shape[0]
    summed = jnp.dot(
        jnp.concatenate([high, low], axis=0), table[6 * INNER :], preferred_element_type=jnp.float32
    )
    summed = summed[:rows_of] + summed[rows_of:]
    mids[...] = summed[:, :INNER] + summed[:, INNER:]

    def copy_out(code):
        e = code // 2
        return pltpu.make_async_copy(result_ref.at[code], own_hbm.at[names[e]], sems.at[code])

    def copy_pair(code):
        to = pair_hbm.at[pair_at + code // 2]
        return pltpu.make_async_copy(result_ref.at[code], to, sems.at[code])

    def columns(code):
        other = held[code // 2, :size].astype(jnp.float32)
        return turned_columns(*split(cross_spectrum(other, wide[code % 2])), table, turn)

    def middle_of(code):
        return mids[pl.ds(lax.rem(code, 2) * 2 * per + code // 2, 1), :]

    def keep_result(code, value):
        result_ref[code] = value

        @pl.when(code % 2 == 0)
        def _():
            copy_out(code).start()

        if pair_hbm is not None:
            @pl.when(code % 2 != 0)
            def _():
                copy_pair(code).start()

    def codes(k):
        return listed[2 * k], listed[jnp.minimum(2 * k + 1, count - 1)]

    def turn_two(k):
        code0, code1 = codes(k)
        kept[...] = jnp.concatenate([*columns(code0), *columns(code1)], axis=0)

    def sum_two(k):
        code0, code1 = codes(k)
        cosine = table[4 * INNER : 6 * INNER, :INNER]
        sine = table[4 * INNER : 6 * INNER, INNER:]
        summed = jnp.dot(kept[:, : 2 * INNER], cosine, preferred_element_type=jnp.float32)
        summed += jnp.dot(kept[:, 2 * INNER :], sine, preferred_element_type=jnp.float32)
        value0 = lags_of(summed[:INNER] + summed[INNER : 2 * INNER], middle_of(code0))
        value1 = lags_of(summed[2 * INNER : 3 * INNER] + summed[3 * INNER :], middle_of(code1))
        return value0, value1

    def keep_two(k, value0, value1):
        code0, code1 = codes(k)
        keep_result(code0, value0)

        @pl.when(2 * k + 1 < count)
        def _():
            keep_result(code1, value1)

    def both(k, _):
        last = jnp.maximum(k - 1, 0)
        values = sum_two(last)
        turn_two(jnp.minimum(k, twos - 1))

        @pl.when(k > 0)
        def _():
            keep_two(last, *values)

        return 0

    twos = (count + 1) // 2
    lax.fori_loop(0, jnp.where(count > 0, twos + 1, 0), both, 0)
    for side, (present, rows) in enumerate(plan):
        for e in range(side * per, (side + 1) * per if present else 0):
            @pl.when(own_w[names[e]] != 0.0)
            def _():
                copy_out(2 * e).wait()

            if rows > 1:
                @pl.when(pair_w[names[e]] != 0.0)
                def _():
                    copy_pair(2 * e + 1).wait()


def stage_call(step, plan, along, slabs, info, own_w, pair_w, mine, tables, own_buf, pair_buf, pair_at, pair_size):
    total = own_w.shape[0]
    count = 2 * CHAINS * slabs[0].shape[0]
    outer = LAGS // INNER
    smem = pl.BlockSpec(memory_space=pltpu.SMEM)
    vmem = pl.BlockSpec(memory_space=pltpu.VMEM)
    hbm = pl.BlockSpec(memory_space=pl.ANY)
    args = [info, own_w, pair_w, *mine, *tables, *slabs]
    specs = [smem] * 3 + [vmem] * (2 + len(tables) + len(slabs))
    used = len(args)
    out_shape = [jax.ShapeDtypeStruct((8, INNER), jnp.float32)]
    out_shape.append(jax.ShapeDtypeStruct((total, outer, INNER), jnp.float32))
    out_specs = [vmem, hbm]
    aliases = {}
    if own_buf is not None:
        aliases[len(args)] = 1
        args.append(own_buf)
        specs.append(hbm)
    with_pair = pair_size is not None
    if with_pair:
        out_shape.append(jax.ShapeDtypeStruct((pair_size, outer, INNER), jnp.float32))
        out_specs.append(hbm)
        if pair_buf is not None:
            aliases[len(args)] = 2
            args.append(pair_buf)
            specs.append(hbm)

    def body(*refs):
        scratch = refs[-8:]
        outs = refs[len(args) : -8]
        pair_ref = outs[2] if with_pair else None
        stage_body(step, plan, along, pair_at, *refs[:used], outs[1], pair_ref, outs[0], *scratch)

    flops = sum(rows * count // 2 for present, rows in plan if present) * 100_000_000
    return pl.pallas_call(
        body,
        out_shape=out_shape,
        in_specs=specs,
        out_specs=out_specs,
        scratch_shapes=[
            pltpu.VMEM((count,) + mine[0].shape, jnp.bfloat16),
            pltpu.VMEM((2, 2 * INNER, mine[0].shape[1]), jnp.float32),
            pltpu.VMEM((2 * count, INNER), jnp.float32),
            pltpu.VMEM((4 * INNER, 2 * mine[0].shape[1]), jnp.bfloat16),
            pltpu.VMEM((2 * count, outer, INNER), jnp.float32),
            pltpu.SMEM((2 * count + 1,), jnp.int32),
            pltpu.SMEM((count,), jnp.int32),
            pltpu.SemaphoreType.DMA((2 * count,)),
        ],
        input_output_aliases=aliases,
        cost_estimate=pl.CostEstimate(flops=flops, bytes_accessed=3_000_000, transcendentals=0),
        compiler_params=pltpu.CompilerParams(vmem_limit_bytes=16 * 1024 * 1024),
    )(*args)


def finish_body(src_ref, own_w, own_ref, early_ref, late_ref, out_ref, lines):
    g = pl.program_id(0)
    first = early_ref.shape[0]
    block, outer = own_ref.shape[:2]
    pitch = outer + 8

    def tile(m, _):
        for k in range(8):
            j = g * block + m * 8 + k
            src = src_ref[j]
            live = own_w[j] != 0.0
            early = early_ref[jnp.clip(src, 0, first - 1)]
            late = late_ref[jnp.clip(src - first, 0, late_ref.shape[0] - 1)]
            value = jnp.where(src < 0, own_ref[m * 8 + k], jnp.where(src < first, early, late))
            lines[pl.ds(k * pitch, outer), :] = jnp.where(live, value, 0.0)
        for n in range(outer):
            to = pl.ds(pl.multiple_of(m * 8 * outer + 8 * n, 8), 8)
            out_ref[to, :] = lines[pl.ds(n, 8, stride=pitch), :]
        return 0

    lax.fori_loop(0, block // 8, tile, 0)


def finish_call(src, own_w, own_buf, early, late):
    outer = LAGS // INNER
    total = src.shape[0]
    block = 32
    smem = pl.BlockSpec(memory_space=pltpu.SMEM)
    vmem = pl.BlockSpec(memory_space=pltpu.VMEM)
    return pl.pallas_call(
        finish_body,
        grid=(total // block,),
        out_shape=jax.ShapeDtypeStruct((total * outer, INNER), jnp.float32),
        in_specs=[smem, smem, pl.BlockSpec((block, outer, INNER), lambda g: (g, 0, 0)), vmem, vmem],
        out_specs=pl.BlockSpec((block * outer, INNER), lambda g: (g, 0)),
        scratch_shapes=[pltpu.VMEM((8 * (outer + 8), INNER), jnp.float32)],
        cost_estimate=pl.CostEstimate(flops=1_000_000, bytes_accessed=8_000_000, transcendentals=0),
        compiler_params=pltpu.CompilerParams(vmem_limit_bytes=16 * 1024 * 1024),
        name="finish",
    )(src, own_w, own_buf, early, late)


def per_device(total, spectra, pair_mask, available):
    along = total // (ACROSS * CORES)
    far = along // 2
    freq = spectra.shape[2]
    column = 2 * freq // INNER
    tables = [jnp.asarray(table) for table in build_tables(freq)]

    def move(value, goal_of):
        pairs = []
        for start in range(total):
            x, z, c = start // (along * CORES), start // CORES % along, start % CORES
            x, z, c = goal_of(x, z, c)
            pairs.append((start, (x % ACROSS * along + z % along) * CORES + c % CORES))
        return lax.ppermute(value, "row", pairs)

    def swap(value):
        return move(value, lambda x, z, c: (x, z, c + 1))

    def onward(value):
        return move(value, lambda x, z, c: (x, z + 1 - 2 * c, c))

    def sideways(value):
        return move(value, lambda x, z, c: (x + 1 - 2 * c, z, c))

    me = lax.axis_index("row")
    x, z, c = me // (along * CORES), me // CORES % along, me % CORES
    info = jnp.stack([x, z, c]).astype(jnp.int32)

    own, *tables = fold_call(spectra.reshape(2 * freq // column, column), tables)
    across = move(own, lambda x, z, c: (x + 2 - 4 * c, z, c))
    flag = lax.dynamic_slice_in_dim(available, me, 1, 0).astype(jnp.float32)
    own_w = pair_mask[0].astype(jnp.float32) * flag * available.astype(jnp.float32)
    pair_w = swap(own_w)
    other = swap(own)
    across, pair_w, other, info = lax.optimization_barrier((across, pair_w, other, info))
    pieces = [own, across, other, swap(across)]
    width = len(pieces) // CHAINS
    slab = tuple(jnp.stack(pieces[n * width : (n + 1) * width]) for n in range(CHAINS))
    mine = (own, other)

    cut = far - 2
    early = late = own_buf = side = None
    for step in range(far + 2):
        plan, slabs = [], []
        for value, stage in ((slab, step), (side, step - 1)):
            plan.append((value is not None, 2 if 0 < stage < far else 1))
            slabs += value or ()
        next_slab, beside = [], []
        for part in slab or ():
            if step < far:
                next_slab.append(onward(part))
        for part in slab or ():
            beside.append(sideways(part))
        side = tuple(beside) or None
        next_slab = tuple(next_slab) or None
        paired = 1 <= step <= far
        if paired and step <= cut:
            buf, at, size = early, 8 * (step - 1), 8 * cut
        elif paired:
            buf, at, size = late, 8 * (step - 1 - cut), 8 * (far - cut)
        else:
            buf, at, size = None, None, None
        token, own_buf, *pair_buf = stage_call(
            step, plan, along, slabs, info, own_w, pair_w, mine, tables, own_buf, buf, at, size
        )
        if paired and step <= cut:
            early = pair_buf[0]
        elif paired:
            late = pair_buf[0]

        def after(parts):
            return parts and tuple(lax.optimization_barrier((part, token))[0] for part in parts)

        slab, side = after(next_slab), side if step > far else after(side)
    early, late = swap(early), swap(late)

    j = lax.iota(jnp.int32, total)
    xj, zj, cj = j // (along * CORES), j // CORES % along, j % CORES
    dx, dz = (xj - x) % ACROSS, (zj - z) % along
    host = (dz < far).astype(jnp.int32)
    stage = jnp.where(dz < far, dz, along - dz)
    beside = dx % 2
    half = jnp.where(beside == 1, (dx + 1 - 2 * host) % ACROSS // 2, dx // 2)
    entry = 4 * beside + 2 * ((cj - host) % CORES) + half
    far_one = (host != c) & (dz != 0) & (dz != far)
    src = jnp.where(far_one, 8 * (stage - 1 + beside) + entry, -1).astype(jnp.int32)
    out = finish_call(src, own_w, own_buf, early, late)
    out = out.reshape(total // 8, LAGS // INNER, 8, INNER)
    return jnp.transpose(out, (0, 2, 1, 3)).reshape(1, total, LAGS)


def solution(mesh):
    total = mesh.shape["row"]

    def program(*args):
        return per_device(total, *args)

    return jax.shard_map(
        program,
        mesh=mesh,
        in_specs=(P(("win", "row"), None, None), P("row", None), P("win")),
        out_specs=P(("win", "row"), None, None),
        check_vma=False,
    )
```

```python
import functools
import math

import jax
import jax.numpy as jnp
import numpy as np
from jax import lax
from jax.experimental import pallas as pl
from jax.experimental.pallas import tpu as pltpu
from jax.sharding import PartitionSpec as P


LAGS = 8192
CORES = 2
ACROSS = 4
INNER = 128
CHAINS = 1


def split_table(table):
    high = table.astype(jnp.bfloat16)
    low = (table - high.astype(np.float64)).astype(jnp.bfloat16)
    return high, low


@functools.cache
def build_tables(freq):
    nfft = 2 * freq
    column = nfft // INNER
    depth = freq // column
    width = column // 2
    outer = LAGS // INNER
    scale = 2.0 / math.sqrt(8.0 * freq)
    lag = np.arange(INNER)[:, None]
    angle = 2.0 * np.pi * ((lag * np.arange(depth)[None, :]) % INNER) / INNER
    after = 2.0 * np.pi * ((lag * (np.arange(depth)[None, :] + 1)) % INNER) / INNER
    section = np.block(
        [
            [np.cos(angle), -np.sin(angle), np.cos(after), -np.sin(after)],
            [np.sin(angle), np.cos(angle), -np.sin(after), -np.cos(after)],
        ]
    )
    first = np.concatenate(split_table(section), axis=0)
    twist = 2.0 * np.pi * ((lag * np.arange(width)[None, :]) % nfft) / nfft
    turn = np.stack([np.cos(twist), np.sin(twist)]).astype(np.float32)
    steps = np.arange(outer)[None, :] - outer // 2
    angle = 2.0 * np.pi * ((np.arange(width)[:, None] * steps) % column) / column
    section = np.concatenate([np.cos(angle), -np.sin(angle)], axis=0) * scale
    second = np.concatenate(split_table(section), axis=1)
    odd = 2 * np.arange(depth)[:, None] + 1
    angle = 2.0 * np.pi * ((odd * lag.T) % (2 * INNER)) / (2 * INNER)
    section = np.concatenate([np.cos(angle), -np.sin(angle)], axis=0) * scale
    middle = np.concatenate(split_table(section), axis=1)
    wide = np.concatenate([second[:width], second[width:]], axis=1)
    return np.concatenate([first, wide, middle], axis=0), turn


def fold_body(whole_ref, out_ref):
    rows, column = whole_ref.shape
    width = column // 2
    whole = whole_ref[...]
    down = lax.broadcasted_iota(jnp.int32, (width, width), 0)
    over = lax.broadcasted_iota(jnp.int32, (width, width), 1)
    mirror = jnp.where(down == lax.rem(width - over, width), 1.0, 0.0).astype(jnp.bfloat16)
    flipped = jnp.dot(whole[:, width:], mirror, preferred_element_type=jnp.float32)
    out_ref[pl.ds(0, rows), :] = whole[:, :width]
    out_ref[pl.ds(rows, rows), :] = flipped.astype(jnp.bfloat16)


def fold_call(whole):
    rows, column = whole.shape
    return pl.pallas_call(
        fold_body,
        out_shape=jax.ShapeDtypeStruct((2 * rows, column // 2), jnp.bfloat16),
        in_specs=[pl.BlockSpec(memory_space=pltpu.VMEM)],
        out_specs=pl.BlockSpec(memory_space=pltpu.VMEM),
        cost_estimate=pl.CostEstimate(flops=1_000_000, bytes_accessed=300_000, transcendentals=0),
        compiler_params=pltpu.CompilerParams(vmem_limit_bytes=16 * 1024 * 1024),
        name="fold",
    )(whole)


def first_column(block):
    over = lax.broadcasted_iota(jnp.int32, (16, block.shape[1]), 1)
    pick = jnp.where(over == 0, 1.0, 0.0).astype(jnp.bfloat16)
    return lax.dot_general(
        pick, block, (((1,), (1,)), ((), ())), preferred_element_type=jnp.float32
    )


def swap_halves(value):
    half = value.shape[1] // 2
    return jnp.concatenate([value[:, half:], value[:, :half]], axis=1)


def split(value):
    high = value.astype(jnp.bfloat16)
    return high, (value - high.astype(jnp.float32)).astype(jnp.bfloat16)


def cross_spectrum(other, mine):
    parts = []
    quarter = mine.shape[0] // 4
    for n in (0, 2):
        ar, ai = mine[n * quarter : (n + 1) * quarter], mine[(n + 1) * quarter : (n + 2) * quarter]
        br, bi = other[n * quarter : (n + 1) * quarter], other[(n + 1) * quarter : (n + 2) * quarter]
        parts += [ar * br + ai * bi, ar * bi - ai * br]
    return jnp.concatenate(parts, axis=0)


def turned_columns(high, low, table, turn):
    wide = jnp.dot(table[: 4 * INNER], high, preferred_element_type=jnp.float32)
    rest = jnp.dot(table[: 2 * INNER], low, preferred_element_type=jnp.float32)
    mixed = wide[: 2 * INNER] + wide[2 * INNER :] + rest
    sr, si = mixed[:INNER], mixed[INNER:]
    tc, ts = turn[0], turn[1]
    turned = jnp.concatenate([sr * tc - si * ts, sr * ts + si * tc], axis=1)
    return split(turned)


def lags_of(summed, middle):
    summed = summed.T
    outer = summed.shape[0] // 2
    parity = lax.broadcasted_iota(jnp.int32, (outer, INNER), 0) % 2
    return summed[:outer] + summed[outer:] + jnp.where(parity == 0, middle, -middle)


def stage_body(step, plan, along, pair_at, info, own_w, pair_w, mine0, mine1, table, turn, *rest):
    chains = CHAINS
    slab_count = chains * sum(present for present, _ in plan)
    slabs, rest = rest[:slab_count], rest[-11:]
    own_hbm, pair_hbm, token, held, wide, mids, kept, result_ref, listed, names, sems = rest
    token[...] = jnp.zeros_like(token)
    x, z, c = info[0], info[1], info[2]
    sign = 2 * c - 1
    part = slabs[0].shape[0]
    per = chains * part
    size = wide.shape[1]
    count = jnp.int32(0)
    taken = 0
    for side, (present, rows) in enumerate(plan):
        if not present:
            continue
        for chain in range(chains):
            held[pl.ds(side * per + chain * part, part)] = slabs[taken][...]
            taken += 1
        zj = lax.rem(z + sign * (step - side) + along, along)
        for n in range(per):
            e = side * per + n
            xj = lax.rem(x + side * sign + 2 * (n % 2) + ACROSS, ACROSS)
            j = (xj * along + zj) * CORES + lax.rem(c + n // 2, CORES)
            names[e] = j
            for row in range(rows):
                listed[count] = e * 2 + row
                keep = (own_w if row == 0 else pair_w)[j] != 0.0
                count = count + keep.astype(jnp.int32)

    quarter = size // 4
    down = lax.broadcasted_iota(jnp.int32, wide.shape[1:], 0)
    over = lax.broadcasted_iota(jnp.int32, wide.shape[1:], 1)
    once = (over == 0) & ((down == 0) | (down == quarter))
    weight = jnp.where(once, 0.5, jnp.where((over == 0) & (down >= 2 * quarter), 0.0, 1.0))
    lane = lax.broadcasted_iota(jnp.int32, (2 * per, INNER), 1)
    spot = lax.broadcasted_iota(jnp.int32, (2 * per, INNER), 0)
    straight = jnp.zeros((2 * per, INNER), jnp.float32)
    for side, (present, rows) in enumerate(plan):
        for e in range(side * per, (side + 1) * per if present else 0):
            edge = first_column(held[e, 2 * quarter :])[: 2 * per]
            straight = jnp.where(spot == e, edge, straight)
    crossed = jnp.where(lane < INNER // 2, 1.0, -1.0) * swap_halves(straight)
    parts = []
    for row in range(2):
        mine = mine1 if row else mine0
        wide[row] = mine[...].astype(jnp.float32) * weight
        edge = first_column(mine[2 * quarter :])[: 2 * per]
        other = swap_halves(edge)
        real = jnp.where(lane < INNER // 2, edge, other)
        imag = jnp.where(lane < INNER // 2, other, edge)
        parts.append(real * straight + imag * crossed)
    high, low = split(jnp.concatenate(parts, axis=0))
    rows_of = high.shape[0]
    summed = jnp.dot(
        jnp.concatenate([high, low], axis=0), table[6 * INNER :], preferred_element_type=jnp.float32
    )
    summed = summed[:rows_of] + summed[rows_of:]
    mids[...] = summed[:, :INNER] + summed[:, INNER:]

    def copy_out(code):
        e = code // 2
        return pltpu.make_async_copy(result_ref.at[code], own_hbm.at[names[e]], sems.at[code])

    def copy_pair(code):
        to = pair_hbm.at[pair_at + code // 2]
        return pltpu.make_async_copy(result_ref.at[code], to, sems.at[code])

    def columns(code):
        other = held[code // 2].astype(jnp.float32)
        return turned_columns(*split(cross_spectrum(other, wide[code % 2])), table, turn)

    def middle_of(code):
        return mids[pl.ds(lax.rem(code, 2) * 2 * per + code // 2, 1), :]

    def keep_result(code, value):
        result_ref[code] = value

        @pl.when(code % 2 == 0)
        def _():
            copy_out(code).start()

        if pair_hbm is not None:
            @pl.when(code % 2 != 0)
            def _():
                copy_pair(code).start()

    def codes(k):
        return listed[2 * k], listed[jnp.minimum(2 * k + 1, count - 1)]

    def turn_two(k):
        code0, code1 = codes(k)
        kept[...] = jnp.concatenate([*columns(code0), *columns(code1)], axis=0)

    def sum_two(k):
        code0, code1 = codes(k)
        cosine = table[4 * INNER : 6 * INNER, :INNER]
        sine = table[4 * INNER : 6 * INNER, INNER:]
        summed = jnp.dot(kept[:, : 2 * INNER], cosine, preferred_element_type=jnp.float32)
        summed += jnp.dot(kept[:, 2 * INNER :], sine, preferred_element_type=jnp.float32)
        value0 = lags_of(summed[:INNER] + summed[INNER : 2 * INNER], middle_of(code0))
        value1 = lags_of(summed[2 * INNER : 3 * INNER] + summed[3 * INNER :], middle_of(code1))
        return value0, value1

    def keep_two(k, value0, value1):
        code0, code1 = codes(k)
        keep_result(code0, value0)

        @pl.when(2 * k + 1 < count)
        def _():
            keep_result(code1, value1)

    def both(k, _):
        last = jnp.maximum(k - 1, 0)
        values = sum_two(last)
        turn_two(jnp.minimum(k, twos - 1))

        @pl.when(k > 0)
        def _():
            keep_two(last, *values)

        return 0

    twos = (count + 1) // 2
    lax.fori_loop(0, jnp.where(count > 0, twos + 1, 0), both, 0)
    for side, (present, rows) in enumerate(plan):
        for e in range(side * per, (side + 1) * per if present else 0):
            @pl.when(own_w[names[e]] != 0.0)
            def _():
                copy_out(2 * e).wait()

            if rows > 1:
                @pl.when(pair_w[names[e]] != 0.0)
                def _():
                    copy_pair(2 * e + 1).wait()


def stage_call(step, plan, along, slabs, info, own_w, pair_w, mine, tables, own_buf, pair_buf, pair_at, pair_size):
    total = own_w.shape[0]
    count = 2 * CHAINS * slabs[0].shape[0]
    outer = LAGS // INNER
    smem = pl.BlockSpec(memory_space=pltpu.SMEM)
    vmem = pl.BlockSpec(memory_space=pltpu.VMEM)
    hbm = pl.BlockSpec(memory_space=pl.ANY)
    args = [info, own_w, pair_w, *mine, *tables, *slabs]
    specs = [smem] * 3 + [vmem] * (2 + len(tables) + len(slabs))
    used = len(args)
    out_shape = [jax.ShapeDtypeStruct((8, INNER), jnp.float32)]
    out_shape.append(jax.ShapeDtypeStruct((total, outer, INNER), jnp.float32))
    out_specs = [vmem, hbm]
    aliases = {}
    if own_buf is not None:
        aliases[len(args)] = 1
        args.append(own_buf)
        specs.append(hbm)
    with_pair = pair_size is not None
    if with_pair:
        out_shape.append(jax.ShapeDtypeStruct((pair_size, outer, INNER), jnp.float32))
        out_specs.append(hbm)
        if pair_buf is not None:
            aliases[len(args)] = 2
            args.append(pair_buf)
            specs.append(hbm)

    def body(*refs):
        scratch = refs[-8:]
        outs = refs[len(args) : -8]
        pair_ref = outs[2] if with_pair else None
        stage_body(step, plan, along, pair_at, *refs[:used], outs[1], pair_ref, outs[0], *scratch)

    flops = sum(rows * count // 2 for present, rows in plan if present) * 100_000_000
    return pl.pallas_call(
        body,
        out_shape=out_shape,
        in_specs=specs,
        out_specs=out_specs,
        scratch_shapes=[
            pltpu.VMEM((count,) + mine[0].shape, jnp.bfloat16),
            pltpu.VMEM((2, 2 * INNER, mine[0].shape[1]), jnp.float32),
            pltpu.VMEM((2 * count, INNER), jnp.float32),
            pltpu.VMEM((4 * INNER, 2 * mine[0].shape[1]), jnp.bfloat16),
            pltpu.VMEM((2 * count, outer, INNER), jnp.float32),
            pltpu.SMEM((2 * count + 1,), jnp.int32),
            pltpu.SMEM((count,), jnp.int32),
            pltpu.SemaphoreType.DMA((2 * count,)),
        ],
        input_output_aliases=aliases,
        cost_estimate=pl.CostEstimate(flops=flops, bytes_accessed=3_000_000, transcendentals=0),
        compiler_params=pltpu.CompilerParams(vmem_limit_bytes=16 * 1024 * 1024),
    )(*args)


def finish_body(src_ref, own_w, own_ref, early_ref, late_ref, out_ref, lines):
    g = pl.program_id(0)
    first = early_ref.shape[0]
    block, outer = own_ref.shape[:2]
    pitch = outer + 8

    def tile(m, _):
        for k in range(8):
            j = g * block + m * 8 + k
            src = src_ref[j]
            live = own_w[j] != 0.0
            early = early_ref[jnp.clip(src, 0, first - 1)]
            late = late_ref[jnp.clip(src - first, 0, late_ref.shape[0] - 1)]
            value = jnp.where(src < 0, own_ref[m * 8 + k], jnp.where(src < first, early, late))
            lines[pl.ds(k * pitch, outer), :] = jnp.where(live, value, 0.0)
        for n in range(outer):
            to = pl.ds(pl.multiple_of(m * 8 * outer + 8 * n, 8), 8)
            out_ref[to, :] = lines[pl.ds(n, 8, stride=pitch), :]
        return 0

    lax.fori_loop(0, block // 8, tile, 0)


def finish_call(src, own_w, own_buf, early, late):
    outer = LAGS // INNER
    total = src.shape[0]
    block = 32
    smem = pl.BlockSpec(memory_space=pltpu.SMEM)
    vmem = pl.BlockSpec(memory_space=pltpu.VMEM)
    return pl.pallas_call(
        finish_body,
        grid=(total // block,),
        out_shape=jax.ShapeDtypeStruct((total * outer, INNER), jnp.float32),
        in_specs=[smem, smem, pl.BlockSpec((block, outer, INNER), lambda g: (g, 0, 0)), vmem, vmem],
        out_specs=pl.BlockSpec((block * outer, INNER), lambda g: (g, 0)),
        scratch_shapes=[pltpu.VMEM((8 * (outer + 8), INNER), jnp.float32)],
        cost_estimate=pl.CostEstimate(flops=1_000_000, bytes_accessed=8_000_000, transcendentals=0),
        compiler_params=pltpu.CompilerParams(vmem_limit_bytes=16 * 1024 * 1024),
        name="finish",
    )(src, own_w, own_buf, early, late)


def per_device(total, spectra, pair_mask, available):
    along = total // (ACROSS * CORES)
    far = along // 2
    freq = spectra.shape[2]
    column = 2 * freq // INNER
    tables = [jnp.asarray(table) for table in build_tables(freq)]

    def move(value, goal_of):
        pairs = []
        for start in range(total):
            x, z, c = start // (along * CORES), start // CORES % along, start % CORES
            x, z, c = goal_of(x, z, c)
            pairs.append((start, (x % ACROSS * along + z % along) * CORES + c % CORES))
        return lax.ppermute(value, "row", pairs)

    def swap(value):
        return move(value, lambda x, z, c: (x, z, c + 1))

    def onward(value):
        return move(value, lambda x, z, c: (x, z + 1 - 2 * c, c))

    def sideways(value):
        return move(value, lambda x, z, c: (x + 1 - 2 * c, z, c))

    me = lax.axis_index("row")
    x, z, c = me // (along * CORES), me // CORES % along, me % CORES
    info = jnp.stack([x, z, c]).astype(jnp.int32)

    own = fold_call(spectra.reshape(2 * freq // column, column))
    across = move(own, lambda x, z, c: (x + 2 - 4 * c, z, c))
    flag = lax.dynamic_slice_in_dim(available, me, 1, 0).astype(jnp.float32)
    own_w = pair_mask[0].astype(jnp.float32) * flag * available.astype(jnp.float32)
    pair_w = swap(own_w)
    other = swap(own)
    across, pair_w, other, info = lax.optimization_barrier((across, pair_w, other, info))
    pieces = [own, across, other, swap(across)]
    width = len(pieces) // CHAINS
    slab = tuple(jnp.stack(pieces[n * width : (n + 1) * width]) for n in range(CHAINS))
    mine = (own, other)

    cut = far - 2
    early = late = own_buf = side = None
    for step in range(far + 2):
        plan, slabs = [], []
        for value, stage in ((slab, step), (side, step - 1)):
            plan.append((value is not None, 2 if 0 < stage < far else 1))
            slabs += value or ()
        next_slab, beside = [], []
        for part in slab or ():
            if step < far:
                next_slab.append(onward(part))
        for part in slab or ():
            beside.append(sideways(part))
        side = tuple(beside) or None
        next_slab = tuple(next_slab) or None
        paired = 1 <= step <= far
        if paired and step <= cut:
            buf, at, size = early, 8 * (step - 1), 8 * cut
        elif paired:
            buf, at, size = late, 8 * (step - 1 - cut), 8 * (far - cut)
        else:
            buf, at, size = None, None, None
        token, own_buf, *pair_buf = stage_call(
            step, plan, along, slabs, info, own_w, pair_w, mine, tables, own_buf, buf, at, size
        )
        if paired and step <= cut:
            early = pair_buf[0]
        elif paired:
            late = pair_buf[0]

        def after(parts):
            return parts and tuple(lax.optimization_barrier((part, token))[0] for part in parts)

        slab, side = after(next_slab), side if step > far else after(side)
    early, late = swap(early), swap(late)

    j = lax.iota(jnp.int32, total)
    xj, zj, cj = j // (along * CORES), j // CORES % along, j % CORES
    dx, dz = (xj - x) % ACROSS, (zj - z) % along
    host = (dz < far).astype(jnp.int32)
    stage = jnp.where(dz < far, dz, along - dz)
    beside = dx % 2
    half = jnp.where(beside == 1, (dx + 1 - 2 * host) % ACROSS // 2, dx // 2)
    entry = 4 * beside + 2 * ((cj - host) % CORES) + half
    far_one = (host != c) & (dz != 0) & (dz != far)
    src = jnp.where(far_one, 8 * (stage - 1 + beside) + entry, -1).astype(jnp.int32)
    out = finish_call(src, own_w, own_buf, early, late)
    out = out.reshape(total // 8, LAGS // INNER, 8, INNER)
    return jnp.transpose(out, (0, 2, 1, 3)).reshape(1, total, LAGS)


def solution(mesh):
    total = mesh.shape["row"]

    def program(*args):
        return per_device(total, *args)

    return jax.shard_map(
        program,
        mesh=mesh,
        in_specs=(P(("win", "row"), None, None), P("row", None), P("win")),
        out_specs=P(("win", "row"), None, None),
        check_vma=False,
    )
```
